256 devices in a mesh: section: 32 (over y, x, z_lo), tensor: 8 (over z_hi, core).
Axes of the slice: x: 4, y: 4, z: 8 (z_hi: 4, z_lo: 2; z = z_hi * 2 + z_lo), core: 2. Of those that a mesh axis runs over, the one named last changes fastest.
Arguments:
- hidden_in: bfloat16 [128, 8192], P(None, 'tensor'), may hold values from -36 to 36
- segment_ids: int32 [4, 32], replicated, may hold values from 0 to 7, never falling along the last dimension, each value on 1 to 8 neighbouring positions
- segment_job: int32 [4, 8], replicated, may hold values from 0 to 5
- job_adapter: int32 [6], replicated, may hold values from 0 to 3
- owner: int32 [32], P('section'), may hold values from 0 to 7
- frozen: bfloat16 [32, 8192, 4096], P('section', None, 'tensor'), may hold values from -0.0625 to 0.0625
- norm_gain: bfloat16 [32, 4096], P('section'), may hold values from 0.3984375 to 1.59375
- inbox_down: bfloat16 [32, 8, 4096, 128], P('section', 'tensor'), may hold values from -0.0625 to 0.0625
- inbox_up: bfloat16 [32, 8, 128, 4096], P('section', 'tensor'), may hold values from -1 to 1
Outputs:
- section_out: bfloat16 [32, 128, 4096], P('section', None, 'tensor')
The draws below stay inside these ranges and needn't reach their ends.
Inputs may be any that keep to these rules, and one draw needn't show every extreme that they name: `segment_ids`: within each micro-batch the segment numbers never fall, and each of the 8 segments has 1 to 8 tokens.
All inputs are finite; a program needn't handle non-finite values.
Results may differ from the reference program's by a relative error of at most 0.02.
Values may be sent and summed in bfloat16 or wider, within the bound.
No kernel may reach another device: no remote copies, remote signals or barrier semaphores. Data moves between devices by JAX's collectives and lax.ppermute only.
A program may use at most 64 MiB of HBM per device.

```python
import math
import jax
import jax.numpy as jnp
import numpy as np
from jax import lax

D = 8192
R = 32
NEW = 4
JOBS = 6
MB = 4
MTOK = 32
SEGS = 8
TOK = 128
PIECE = 512
SEG_MOST = 8
N_SECTION = 32
N_TENSOR = 8


def draw_hidden_in(key, part):
    base_key, col_key, row_key = jax.random.split(key, 3)
    col_scale = jnp.exp(jax.random.uniform(col_key, (1, D), jnp.float32, math.log(0.3), math.log(3.0)))
    row_scale = jnp.exp(jax.random.uniform(row_key, (TOK, 1), jnp.float32, math.log(0.3), math.log(3.0)))
    values = jnp.clip(jax.random.normal(base_key, (TOK, D), jnp.float32), -4.0, 4.0)
    return (values * col_scale * row_scale).astype(jnp.bfloat16)


def place_ends(result, stream_key, smallest, top_value):
    dims = result.shape
    index_at = [jax.random.randint(jax.random.fold_in(stream_key, axis), (), 0, dims[axis]) for axis in range(len(dims))]
    result = result.at[tuple(index_at)].set(smallest)
    longest = dims.index(max(dims))
    index_at[longest] = (index_at[longest] + 1) % dims[longest]
    return result.at[tuple(index_at)].set(top_value)


def steps_of(key, shape, shards, low, largest):
    def one(position, shards_of):
        draws = jax.random.uniform(jax.random.fold_in(jax.random.fold_in(key, 6), position), (shards_of,), jnp.float32, low / len(shards), largest / len(shards))
        return jnp.repeat(jnp.exp(draws), shape[position] // shards_of).reshape((-1,) + (1,) * (len(shape) - position - 1))

    loudness = one(*shards[0])
    for cut in shards[1:]:
        loudness = loudness * one(*cut)
    return loudness


def split_up(amount, total, reach, lean):
    weights = [(1 << 20) // math.isqrt(standing ** lean) + 1 for standing in range(2, amount + 1)]
    rest, holding = total - reach - (amount - 1), [1] * (amount - 1)
    while rest > 0:
        free = [i for i in range(amount - 1) if holding[i] < reach]
        whole, budget = sum([weights[i] for i in free]), rest
        for i in free:
            extra = min(reach - holding[i], max(1, budget * weights[i] // whole), rest)
            holding[i] = holding[i] + extra
            rest = rest - extra
    return np.array([reach] + holding)


def uneven_parts(stream_key, count, total, most, skew):
    if count == 2:
        one = jax.random.randint(stream_key, (), max(1, total - most), min(most, total - 1) + 1)
        return jnp.stack([one, total - one])
    lengths = jnp.asarray(split_up(count, total, most, skew), jnp.int32)
    couples = (count - 1) // 2
    giver, taker = lengths[1:1 + 2 * couples:2], lengths[2:2 + 2 * couples:2]
    room = jnp.minimum(giver - 1, most - taker)
    passed = jax.random.randint(jax.random.fold_in(stream_key, 1), (couples,), 0, 1 << 20) % (room + 1)
    lengths = lengths.at[1:1 + 2 * couples:2].set(giver - passed).at[2:2 + 2 * couples:2].set(taker + passed)
    return lengths[jax.random.permutation(jax.random.fold_in(stream_key, 2), count)]


def gaussian(stream_key, shape, scale, reach, cuts=(), kind=jnp.bfloat16):
    loudness = steps_of(stream_key, shape, cuts, -0.22, 0.18) if cuts else 1.0
    result = jax.random.normal(stream_key, shape, jnp.float32) * scale * loudness
    return jnp.minimum(jnp.maximum(result, -reach), reach).astype(kind)


def setup_inputs(seed: int = 0) -> dict:
    key_list = jax.random.split(jax.random.key(seed), 10)
    hidden_in = draw_hidden_in(jax.random.fold_in(key_list[9], 71), 0)
    segment_ids = jax.vmap(lambda own: jnp.searchsorted(jnp.cumsum(uneven_parts(own, SEGS, MTOK, SEG_MOST, 2)), jnp.arange(MTOK), side="right"))(jax.random.split(key_list[1], MB)).reshape((MB, MTOK)).astype(jnp.int32)
    segment_job = place_ends(jax.random.randint(key_list[2], (MB, SEGS), 0, JOBS), jax.random.fold_in(key_list[2], 1), 0, JOBS - 1).astype(jnp.int32)
    job_adapter = place_ends(jax.random.randint(key_list[3], (JOBS,), 0, NEW), jax.random.fold_in(key_list[3], 1), 0, NEW - 1).astype(jnp.int32)
    owner = place_ends(jax.random.randint(key_list[4], (N_SECTION,), 0, N_TENSOR), jax.random.fold_in(key_list[4], 1), 0, N_TENSOR - 1).astype(jnp.int32)
    frozen = gaussian(key_list[5], (N_SECTION, D, D // 2), D ** -0.5, 0.0625, ((0, 32), (2, 8)))
    norm_gain = jnp.clip(1.0 + 0.12 * jax.random.normal(key_list[6], (N_SECTION, D // 2), jnp.float32), 0.3984375, 1.59375).astype(jnp.bfloat16)
    inbox_down = gaussian(key_list[7], (N_SECTION, N_TENSOR, D // 2, NEW * R), D ** -0.5, 0.0625, ((0, 32), (1, 8)))
    inbox_up = gaussian(key_list[8], (N_SECTION, N_TENSOR, NEW * R, D // 2), R ** -0.5, 1.0, ((0, 32), (1, 8)))
    return dict(hidden_in=hidden_in, segment_ids=segment_ids, segment_job=segment_job, job_adapter=job_adapter, owner=owner, frozen=frozen, norm_gain=norm_gain, inbox_down=inbox_down, inbox_up=inbox_up)


epsilon = 1e-05

def alternate(lower_part, upper_part):
    lead_rows = lower_part.shape[0]
    blocks = jnp.stack([lower_part.reshape(lead_rows, N_TENSOR, PIECE), upper_part.reshape(lead_rows, N_TENSOR, PIECE)], axis=2)
    return blocks.reshape(lead_rows, 2 * N_TENSOR * PIECE)

def product(left, right):
    return jnp.dot(left, right, preferred_element_type=jnp.float32)

def reference(hidden_in, segment_ids, segment_job, job_adapter, owner, frozen, norm_gain, inbox_down, inbox_up):
    token_job = jnp.take_along_axis(segment_job, segment_ids, axis=1)
    token_adapter = jnp.take(job_adapter, token_job.reshape(TOK), axis=0)
    keep_mask = jnp.arange(NEW * R, dtype=jnp.int32)[None, :] // R == token_adapter[:, None]
    state_now = hidden_in
    pieces = []
    for section_level in range(N_SECTION // 2):
        low_index = 2 * section_level
        high_index = low_index + 1
        weight = alternate(frozen[low_index], frozen[high_index])
        down_rows = alternate(inbox_down[low_index, owner[low_index]].T, inbox_down[high_index, owner[high_index]].T).T
        up_cols = alternate(inbox_up[low_index, owner[low_index]], inbox_up[high_index, owner[high_index]])
        gain_row = alternate(norm_gain[low_index][None, :], norm_gain[high_index][None, :])[0]
        values = state_now.astype(jnp.float32)
        row_scale = lax.rsqrt(lax.optimization_barrier(jnp.mean(values * values, axis=1, keepdims=True)) + epsilon)
        normed = (values * row_scale * gain_row.astype(jnp.float32)).astype(jnp.bfloat16)
        projected = product(normed, down_rows)
        kept_rank = jnp.where(keep_mask, projected, 0.0).astype(jnp.bfloat16)
        state_now = (values + product(normed, weight) + product(kept_rank, up_cols)).astype(jnp.bfloat16)
        split_state = state_now.reshape(TOK, N_TENSOR, 2, PIECE)
        pieces.append(split_state[:, :, 0, :].reshape(TOK, N_TENSOR * PIECE))
        pieces.append(split_state[:, :, 1, :].reshape(TOK, N_TENSOR * PIECE))
    return jnp.stack(pieces, axis=0)
```

```python
import functools

import jax
import jax.numpy as jnp
from jax import lax
from jax.experimental import pallas as pl
from jax.experimental.pallas import tpu as pltpu
from jax.sharding import PartitionSpec as P

R = 32
LANES = 128
SUB = 8
epsilon = 1e-05
AXES = ("section", "tensor")


def routed(value, levels, chips, route):
    def place(level, chip, core):
        section = 2 * (level % levels) + chip % 2
        return section * chips + (chip % chips) // 2 * 2 + core

    pairs = []
    for level in range(levels):
        for chip in range(chips):
            for core in range(2):
                target = route(level, chip, core)
                if target is not None:
                    pairs.append((place(level, chip, core), place(*target)))
    return lax.ppermute(value, AXES, pairs)


def bring(near_a, near_b, sent):
    def kernel(a, b, sent, out_a, out_b, done):
        copies = [pltpu.make_async_copy(a, out_a, done.at[0]), pltpu.make_async_copy(b, out_b, done.at[1])]
        for copy in copies:
            copy.start()
        for copy in copies:
            copy.wait()

    return pl.pallas_call(
        kernel,
        out_shape=tuple(pltpu.VMEM(x.shape, x.dtype) for x in (near_a, near_b)),
        in_specs=[pl.BlockSpec(memory_space=pl.ANY)] * 3,
        out_specs=(pl.BlockSpec(memory_space=pltpu.VMEM),) * 2,
        scratch_shapes=[pltpu.SemaphoreType.DMA((2,))],
        compiler_params=pltpu.CompilerParams(vmem_limit_bytes=1 << 20),
        cost_estimate=pl.CostEstimate(flops=1 << 32, bytes_accessed=4 * near_a.size, transcendentals=0),
        name="bring",
    )(near_a, near_b, sent)


def dot(left, right):
    return jnp.dot(left, right, preferred_element_type=jnp.float32)


def partial_kernel(rows, order, more, static, *refs):
    blocks_in, (gain, own_w, other_w), out = refs[: len(order)], refs[len(order) : len(order) + 3], refs[-1]
    core = static[4]
    cols = own_w.shape[2]
    blocks = 2 * cols // LANES
    own_sum = other_sum = squares = low = None
    for k, block in zip(order, blocks_in):
        place = static[k]
        parts = []
        for j in range(blocks):
            x = block[j * rows : (j + 1) * rows, :].astype(jnp.float32)
            squares = x * x if squares is None else squares + x * x
            parts.append((x * gain[place, j : j + 1, :]).astype(jnp.bfloat16))
        scaled = jnp.concatenate(parts, axis=1)
        low_k = block[blocks * rows :, :].astype(jnp.float32)
        own_k = dot(scaled, own_w[place])
        other_k = dot(scaled, other_w[place])
        own_sum = own_k if own_sum is None else own_sum + own_k
        other_sum = other_k if other_sum is None else other_sum + other_k
        low = low_k if low is None else low + low_k
    own_at = pl.ds(pl.multiple_of(core * rows, SUB), rows)
    other_at = pl.ds(pl.multiple_of((1 - core) * rows, SUB), rows)
    total = jnp.broadcast_to(jnp.sum(squares, axis=1, keepdims=True), (rows, LANES))
    if more:
        before = refs[len(order) + 3]
        own_sum = own_sum + before[own_at, :]
        other_sum = other_sum + before[other_at, :]
        low = low + before[2 * rows : 2 * rows + SUB, 0:LANES]
    out[own_at, :] = own_sum
    out[other_at, :] = other_sum
    out[2 * rows : 2 * rows + SUB, 0:LANES] = low
    for g in range(rows // SUB):
        at = slice(2 * rows + SUB, 2 * rows + 2 * SUB), slice(g * LANES, (g + 1) * LANES)
        part = total[g * SUB : (g + 1) * SUB]
        out[at] = part + before[at] if more else part


def finish_kernel(
    rows, units, levels, width, static, turn, own_e, far_e, own_x, far_x, slot, up, down, source, results_in, sent, results
):
    core, level = static[4], static[5]
    step = turn[0]
    cols = own_e.shape[1]
    blocks = 2 * cols // LANES
    groups = rows // SUB
    behind = step - level
    active = jnp.logical_and(behind >= 0, jnp.logical_and(behind < 2 * units, behind % 2 == 0))
    feeding = jnp.logical_and(level == levels - 1, jnp.logical_and(step % 2 != 0, step + 1 < 2 * units))
    unit = jnp.where(feeding, (step + 1) // 2, jnp.clip(behind // 2, 0, units - 1))
    at = pl.multiple_of(unit * rows, SUB)
    token_slot = slot[pl.ds(at, rows), :]
    lane_slot = lax.broadcasted_iota(jnp.int32, (SUB, LANES), 1) // R
    low = own_e[2 * rows : 2 * rows + SUB, 0:LANES] + far_e[2 * rows : 2 * rows + SUB, 0:LANES]
    turned = [low] + [pltpu.roll(low, s * R, 1) for s in range(1, 4)]
    scales, kept = [], []
    for g in range(groups):
        here = pl.ds(g * LANES, LANES)
        squares = own_e[2 * rows + SUB : 2 * rows + 2 * SUB, here] + far_e[2 * rows + SUB : 2 * rows + 2 * SUB, here]
        scale = lax.rsqrt(squares / width + epsilon)
        spread = turned[(0 - g) % 4]
        for a in range(1, 4):
            spread = jnp.where(lane_slot == a, turned[(a - g) % 4], spread)
        mine = lane_slot == token_slot[g * SUB : (g + 1) * SUB]
        kept.append(jnp.where(mine, spread * scale, 0.0))
        scales.append(scale)
    scale = jnp.concatenate(scales, axis=0)
    kept = jnp.concatenate(kept, axis=0).astype(jnp.bfloat16)
    fresh = []
    first = core == 0
    for j in range(blocks):
        row = j * rows
        x = jnp.where(first, own_x[row : row + rows, :], far_x[row : row + rows, :]).astype(jnp.float32)
        half, lane = (0, j * LANES) if j * LANES < cols else (rows, j * LANES - cols)
        product = own_e[half : half + rows, lane : lane + LANES] + far_e[half : half + rows, lane : lane + LANES]
        added = dot(kept, up[j * LANES : (j + 1) * LANES, :])
        y = (x + scale * product + added).astype(jnp.bfloat16)
        fed = source[pl.ds(pl.multiple_of(unit * (blocks * rows) + row, SUB), rows), :]
        fresh.append(jnp.where(feeding, fed, y))
    for j in range(blocks):
        sent[j * rows : (j + 1) * rows, :] = fresh[j]
    next_low = dot(jnp.concatenate(fresh, axis=1), down[...])
    packed = None
    for g in range(groups):
        mine = lane_slot == token_slot[g * SUB : (g + 1) * SUB]
        picked = jnp.where(mine, next_low[g * SUB : (g + 1) * SUB], 0.0)
        picked = picked + pltpu.roll(picked, 2 * R, 1)
        picked = picked + pltpu.roll(picked, R, 1)
        packed = picked if packed is None else jnp.where(lane_slot == g, picked, packed)
    sent[blocks * rows :, :] = packed.astype(jnp.bfloat16)

    @pl.when(active)
    def _():
        for i in range(blocks // 2):
            mine = jnp.where(first, fresh[i], fresh[blocks // 2 + i])
            results[pl.ds(at, rows), i * LANES : (i + 1) * LANES] = mine


def local(
    hidden_in, segment_ids, segment_job, job_adapter, owner, frozen, norm_gain, inbox_down, inbox_up
):
    chips = lax.axis_size("tensor")
    levels = lax.axis_size("section") // 2
    cols = frozen.shape[2]
    half_width = norm_gain.shape[1]
    units, rows = segment_ids.shape
    quads = chips // 2
    pair = 2 * cols
    blocks = pair // LANES
    position = lax.axis_index("section")
    side, level = position % 2, position // 2
    shard = lax.axis_index("tensor")
    spot, core = shard // 2, shard % 2
    first = core == 0
    move = functools.partial(routed, levels=levels, chips=chips)

    def swap(value):
        return move(value, route=lambda p, z, c: (p, z, 1 - c))

    down = inbox_down[0, 0]
    up = inbox_up[0, 0].reshape(LANES, half_width // LANES, LANES).transpose(1, 0, 2).reshape(half_width, LANES)
    from_core = swap(jnp.where(first, down, up))
    chip_has = jnp.where(owner[0] % 2 == core, jnp.where(first, up, down), from_core)
    owner_next = move(owner, route=lambda p, z, c: (p - 1, z, c))
    gain_next = move(norm_gain, route=lambda p, z, c: (p - 1, z, c))
    gain_other = move(norm_gain, route=lambda p, z, c: (p, z ^ 1, c))
    wanted = jnp.where(first, owner[0], owner_next[0]) // 2
    adapter_part = None
    chunks = [lax.dynamic_slice_in_dim(chip_has, (spot + k) % quads * pair, pair, 0) for k in range(quads)]
    chunks, columns = lax.optimization_barrier((chunks, frozen[0]))
    for k in (2, 1, 3, 0):
        came = move(chunks[k], route=lambda p, z, c, k=k: (p - c, z + 2 * k, c))
        hit = (spot - k) % quads == wanted
        adapter_part = came if adapter_part is None else jnp.where(hit, came, adapter_part)
    adapter_other = swap(adapter_part)
    up_pair = jnp.where(first, adapter_part, adapter_other)
    down_pair = jnp.where(first, adapter_other, adapter_part)
    gain_rows = lax.dynamic_slice_in_dim(gain_next[0], spot * pair, pair, 0).astype(jnp.float32)
    down_pair = (down_pair.astype(jnp.float32) * gain_rows[:, None]).astype(jnp.bfloat16)
    gain = jnp.where(first, norm_gain, gain_other).reshape(quads, blocks, LANES).astype(jnp.float32)

    by_side = columns.reshape(quads, 2, 2, cols, cols)
    arriving = (side + core) % 2
    own_w = lax.dynamic_index_in_dim(by_side, arriving, 2, keepdims=False).reshape(quads, pair, cols)
    far_w = lax.dynamic_index_in_dim(by_side, 1 - arriving, 2, keepdims=False).reshape(quads, pair, cols)
    other_w = swap(far_w)

    own_half = lax.dynamic_slice_in_dim(hidden_in, side * cols, cols, 1)
    other_half = swap(own_half)
    both = jnp.concatenate([jnp.where(first, own_half, other_half), jnp.where(first, other_half, own_half)], axis=1)
    source = both.reshape(units, rows, blocks, LANES).transpose(0, 2, 1, 3).reshape(units * blocks * rows, LANES)

    seg_hit = segment_ids[:, :, None] == lax.broadcasted_iota(jnp.int32, (1, 1, segment_job.shape[1]), 2)
    token_job = jnp.sum(jnp.where(seg_hit, segment_job[:, None, :], 0), axis=2)
    job_hit = token_job[:, :, None] == lax.broadcasted_iota(jnp.int32, (1, 1, job_adapter.shape[0]), 2)
    token_slot = jnp.sum(jnp.where(job_hit, job_adapter[None, None, :], 0), axis=2)
    slot = jnp.broadcast_to(token_slot.reshape(units * rows, 1), (units * rows, LANES))
    slot = lax.optimization_barrier(slot)

    places = [(spot - k - core * (1 - side)) % quads for k in range(quads)]
    static = jnp.stack(places + [core, level]).astype(jnp.int32)

    smem = pl.BlockSpec(memory_space=pltpu.SMEM)
    vmem = pl.BlockSpec(memory_space=pltpu.VMEM)
    payload = jax.ShapeDtypeStruct((blocks * rows + SUB, LANES), jnp.bfloat16)
    partial = jax.ShapeDtypeStruct((2 * rows + 2 * SUB, cols), jnp.float32)
    out_shape = jax.ShapeDtypeStruct((units * rows, cols), jnp.bfloat16)
    early, late = (2, 1), (3, 0)

    def multiply(order, more):
        return pl.pallas_call(
            functools.partial(partial_kernel, rows, order, more),
            out_shape=partial,
            in_specs=[smem] + [vmem] * (len(order) + 3 + more),
            out_specs=vmem,
            compiler_params=pltpu.CompilerParams(vmem_limit_bytes=16 << 20),
            cost_estimate=pl.CostEstimate(
                flops=len(order) * 2 * rows * pair * pair, bytes_accessed=len(order) * 2 * pair * pair, transcendentals=0
            ),
            name="multiply",
        )

    finish = pl.pallas_call(
        functools.partial(finish_kernel, rows, units, levels, 2 * half_width),
        out_shape=(payload, out_shape),
        in_specs=[smem, smem] + [vmem] * 9,
        out_specs=(vmem, vmem),
        input_output_aliases={10: 1},
        compiler_params=pltpu.CompilerParams(vmem_limit_bytes=16 << 20),
        name="finish",
    )

    def end(step, own_e, far_e, own_x, far_x, results):
        turn = jnp.full((1,), step, jnp.int32)
        return finish(static, turn, own_e, far_e, own_x, far_x, slot, up_pair, down_pair, source, results)

    def half_step(step, parity, sent, results):
        blocks_in = {
            k: move(sent, route=lambda p, z, c, k=k: (p + 1, z + 2 * k + c, c) if p % 2 == parity else None)
            for k in early + late
        }
        far_x = swap(blocks_in[0])
        weights = gain, *bring(own_w, other_w, sent)
        own_e = multiply(early, False)(static, *[blocks_in[k] for k in early], *weights)
        own_e = multiply(late, True)(static, *[blocks_in[k] for k in late], *weights, own_e)
        far_e = swap(own_e)
        return end(step, own_e, far_e, blocks_in[0], far_x, results)

    nothing_e = jnp.zeros(partial.shape, partial.dtype)
    nothing_x = jnp.zeros(payload.shape, payload.dtype)
    carry = end(-1, nothing_e, nothing_e, nothing_x, nothing_x, jnp.zeros(out_shape.shape, out_shape.dtype))

    def two_steps(i, carry):
        carry = half_step(2 * i, 1, *carry)
        return half_step(2 * i + 1, 0, *carry)

    _, results = lax.fori_loop(0, (levels + 2 * units - 2) // 2, two_steps, carry)
    return results[None]


def solution(mesh):
    return jax.shard_map(
        local,
        mesh=mesh,
        in_specs=(
            P(None, "tensor"),
            P(),
            P(),
            P(),
            P("section"),
            P("section", None, "tensor"),
            P("section", None),
            P("section", "tensor", None, None),
            P("section", "tensor", None, None),
        ),
        out_specs=P("section", None, "tensor"),
        check_vma=False,
    )
```

```python
import functools

import jax
import jax.numpy as jnp
from jax import lax
from jax.experimental import pallas as pl
from jax.experimental.pallas import tpu as pltpu
from jax.sharding import PartitionSpec as P

R = 32
LANES = 128
SUB = 8
epsilon = 1e-05
row = 4
AXES = ("section", "tensor")


def routed(value, levels, chips, route):
    def place(level, chip, core):
        section = 2 * (level % levels) + chip % 2
        return section * chips + (chip % chips) // 2 * 2 + core

    pairs = []
    for level in range(levels):
        for chip in range(chips):
            for core in range(2):
                target = route(level, chip, core)
                if target is not None:
                    pairs.append((place(level, chip, core), place(*target)))
    return lax.ppermute(value, AXES, pairs)


def bring(columns, far_w, static, sent, parity):
    quads, cores, _, cols, _ = columns.shape

    def kernel(static, columns, far_w, sent, out_a, out_b, done):
        copies = [pltpu.make_async_copy(far_w, out_b, done.at[quads * cores])]
        for q in range(quads):
            for core in range(cores):
                source = columns.at[q, core, static[6]]
                target = out_a.at[q, pl.ds(core * cols, cols), :]
                copies.append(pltpu.make_async_copy(source, target, done.at[q * cores + core]))

        @pl.when(static[5] & 1 != parity)
        def _():
            for copy in copies:
                copy.start()
            for copy in copies:
                copy.wait()

    held = pltpu.VMEM(far_w.shape, far_w.dtype)
    return pl.pallas_call(
        kernel,
        out_shape=(held, held),
        in_specs=[pl.BlockSpec(memory_space=pltpu.SMEM)] + [pl.BlockSpec(memory_space=pl.ANY)] * 3,
        out_specs=(pl.BlockSpec(memory_space=pltpu.VMEM),) * 2,
        scratch_shapes=[pltpu.SemaphoreType.DMA((quads * cores + 1,))],
        compiler_params=pltpu.CompilerParams(vmem_limit_bytes=1 << 20),
        cost_estimate=pl.CostEstimate(flops=1 << 32, bytes_accessed=4 * far_w.size, transcendentals=0),
        name="bring",
    )(static, columns, far_w, sent)


def stage(columns, static, after):
    quads, cores, _, cols, _ = columns.shape

    def kernel(static, columns, after, out, held, came, went):
        inward, outward = [], []
        for q in range(quads):
            for core in range(cores):
                i = q * cores + core
                rows_at = pl.ds(core * cols, cols)
                source = columns.at[q, core, 1 - static[6]]
                inward.append(pltpu.make_async_copy(source, held.at[q, rows_at, :], came.at[i]))
                outward.append(pltpu.make_async_copy(held.at[q, rows_at, :], out.at[q, rows_at, :], went.at[i]))
        for copy in inward:
            copy.start()
        for copy, onward in zip(inward, outward):
            copy.wait()
            onward.start()
        for onward in outward:
            onward.wait()

    return pl.pallas_call(
        kernel,
        out_shape=jax.ShapeDtypeStruct((quads, cores * cols, cols), columns.dtype),
        in_specs=[pl.BlockSpec(memory_space=pltpu.SMEM)] + [pl.BlockSpec(memory_space=pl.ANY)] * 2,
        out_specs=pl.BlockSpec(memory_space=pl.ANY),
        scratch_shapes=[
            pltpu.VMEM((quads, cores * cols, cols), columns.dtype),
            pltpu.SemaphoreType.DMA((quads * cores,)),
            pltpu.SemaphoreType.DMA((quads * cores,)),
        ],
        compiler_params=pltpu.CompilerParams(vmem_limit_bytes=8 << 20),
        cost_estimate=pl.CostEstimate(flops=1 << 32, bytes_accessed=columns.size, transcendentals=0),
        name="stage",
    )(static, columns, after)


def dot(left, right):
    return jnp.dot(left, right, preferred_element_type=jnp.float32)


def partial_kernel(rows, order, more, parity, static, *refs):
    @pl.when(static[5] & 1 != parity)
    def _():
        partial_body(rows, order, more, static, *refs)


def partial_body(rows, order, more, static, *refs):
    blocks_in, (gain, own_w, other_w), out = refs[: len(order)], refs[len(order) : len(order) + 3], refs[-1]
    core = static[4]
    cols = own_w.shape[2]
    blocks = 2 * cols // LANES
    own_sum = other_sum = squares = low = None
    for k, block in zip(order, blocks_in):
        place = static[k]
        parts = []
        for j in range(blocks):
            x = block[j * rows : (j + 1) * rows, :].astype(jnp.float32)
            squares = x * x if squares is None else squares + x * x
            parts.append((x * gain[place, j : j + 1, :]).astype(jnp.bfloat16))
        scaled = jnp.concatenate(parts, axis=1)
        low_k = block[blocks * rows :, :].astype(jnp.float32)
        own_k = dot(scaled, own_w[place])
        other_k = dot(scaled, other_w[place])
        own_sum = own_k if own_sum is None else own_sum + own_k
        other_sum = other_k if other_sum is None else other_sum + other_k
        low = low_k if low is None else low + low_k
    own_at = pl.ds(pl.multiple_of(core * rows, SUB), rows)
    other_at = pl.ds(pl.multiple_of((1 - core) * rows, SUB), rows)
    total = jnp.broadcast_to(jnp.sum(squares, axis=1, keepdims=True), (rows, LANES))
    if more:
        before = refs[len(order) + 3]
        own_sum = own_sum + before[own_at, :]
        other_sum = other_sum + before[other_at, :]
        low = low + before[2 * rows : 2 * rows + SUB, 0:LANES]
    out[own_at, :] = own_sum
    out[other_at, :] = other_sum
    out[2 * rows : 2 * rows + SUB, 0:LANES] = low
    for g in range(rows // SUB):
        at = slice(2 * rows + SUB, 2 * rows + 2 * SUB), slice(g * LANES, (g + 1) * LANES)
        part = total[g * SUB : (g + 1) * SUB]
        out[at] = part + before[at] if more else part


def finish_kernel(rows, units, levels, width, parity, static, *refs):
    @pl.when(static[5] & 1 != parity)
    def _():
        finish_body(rows, units, levels, width, static, *refs)


def finish_body(
    rows, units, levels, width, static, turn, own_e, far_e, own_x, far_x, slot, up, down, source, results_in, sent, results
):
    core, level = static[4], static[5]
    step = turn[0]
    cols = own_e.shape[1]
    blocks = 2 * cols // LANES
    groups = rows // SUB
    behind = step - level
    active = jnp.logical_and(behind >= 0, jnp.logical_and(behind < 2 * units, behind % 2 == 0))
    feeding = jnp.logical_and(level == levels - 1, jnp.logical_and(step % 2 != 0, step + 1 < 2 * units))
    unit = jnp.where(feeding, (step + 1) // 2, jnp.clip(behind // 2, 0, units - 1))
    at = pl.multiple_of(unit * rows, SUB)
    token_slot = slot[pl.ds(at, rows), :]
    lane_slot = lax.broadcasted_iota(jnp.int32, (SUB, LANES), 1) // R
    low = own_e[2 * rows : 2 * rows + SUB, 0:LANES] + far_e[2 * rows : 2 * rows + SUB, 0:LANES]
    turned = [low] + [pltpu.roll(low, s * R, 1) for s in range(1, 4)]
    scales, kept = [], []
    for g in range(groups):
        here = pl.ds(g * LANES, LANES)
        squares = own_e[2 * rows + SUB : 2 * rows + 2 * SUB, here] + far_e[2 * rows + SUB : 2 * rows + 2 * SUB, here]
        scale = lax.rsqrt(squares / width + epsilon)
        spread = turned[(0 - g) % 4]
        for a in range(1, 4):
            spread = jnp.where(lane_slot == a, turned[(a - g) % 4], spread)
        mine = lane_slot == token_slot[g * SUB : (g + 1) * SUB]
        kept.append(jnp.where(mine, spread * scale, 0.0))
        scales.append(scale)
    scale = jnp.concatenate(scales, axis=0)
    kept = jnp.concatenate(kept, axis=0).astype(jnp.bfloat16)
    fresh = []
    first = core == 0
    for j in range(blocks):
        row = j * rows
        x = jnp.where(first, own_x[row : row + rows, :], far_x[row : row + rows, :]).astype(jnp.float32)
        half, lane = (0, j * LANES) if j * LANES < cols else (rows, j * LANES - cols)
        product = own_e[half : half + rows, lane : lane + LANES] + far_e[half : half + rows, lane : lane + LANES]
        added = dot(kept, up[j * LANES : (j + 1) * LANES, :])
        y = (x + scale * product + added).astype(jnp.bfloat16)
        fed = source[pl.ds(pl.multiple_of(unit * (blocks * rows) + row, SUB), rows), :]
        fresh.append(jnp.where(feeding, fed, y))
    for j in range(blocks):
        sent[j * rows : (j + 1) * rows, :] = fresh[j]
    next_low = dot(jnp.concatenate(fresh, axis=1), down[...])
    packed = None
    for g in range(groups):
        mine = lane_slot == token_slot[g * SUB : (g + 1) * SUB]
        picked = jnp.where(mine, next_low[g * SUB : (g + 1) * SUB], 0.0)
        picked = picked + pltpu.roll(picked, 2 * R, 1)
        picked = picked + pltpu.roll(picked, R, 1)
        packed = picked if packed is None else jnp.where(lane_slot == g, picked, packed)
    sent[blocks * rows :, :] = packed.astype(jnp.bfloat16)

    @pl.when(active)
    def _():
        for i in range(blocks // 2):
            mine = jnp.where(first, fresh[i], fresh[blocks // 2 + i])
            results[pl.ds(at, rows), i * LANES : (i + 1) * LANES] = mine


def relay(
    hidden_in, segment_ids, segment_job, job_adapter, owner, frozen, norm_gain, inbox_down, inbox_up
):
    chips = lax.axis_size("tensor")
    levels = lax.axis_size("section") // 2
    cols = frozen.shape[2]
    half_width = norm_gain.shape[1]
    units, rows = segment_ids.shape
    quads = chips // 2
    pair = 2 * cols
    blocks = pair // LANES
    position = lax.axis_index("section")
    side, level = position & 1, position >> 1
    shard = lax.axis_index("tensor")
    spot, core = shard >> 1, shard & 1
    first = core == 0
    move = functools.partial(routed, levels=levels, chips=chips)

    def swap(value):
        return move(value, route=lambda p, z, c: (p, z, 1 - c))

    arriving = side ^ core
    places = [(spot - k - core * (1 - side)) & (quads - 1) for k in range(quads)]
    static = jnp.stack(places + [core, level, arriving]).astype(jnp.int32)

    down = inbox_down[0, 0]
    up = inbox_up[0, 0].reshape(LANES, half_width // LANES, LANES).transpose(1, 0, 2).reshape(half_width, LANES)
    from_core = swap(jnp.where(first, down, up))
    chip_has = jnp.where(owner[0] & 1 == core, jnp.where(first, up, down), from_core)
    owner_next = move(owner, route=lambda p, z, c: (p - 1, z, c))
    gain_next = move(norm_gain, route=lambda p, z, c: (p - 1, z, c))
    gain_other = move(norm_gain, route=lambda p, z, c: (p, z ^ 1, c))
    wanted = jnp.where(first, owner[0], owner_next[0]) >> 1
    adapter_part = None
    chunks = [lax.dynamic_slice_in_dim(chip_has, ((spot + k) & (quads - 1)) * pair, pair, 0) for k in range(quads)]
    for k in (2, 1, 3, 0):
        came = move(chunks[k], route=lambda p, z, c, k=k: (p - c, z + 2 * k, c))
        hit = (spot - k) & (quads - 1) == wanted
        adapter_part = came if adapter_part is None else jnp.where(hit, came, adapter_part)
    adapter_other = swap(adapter_part)
    up_pair = jnp.where(first, adapter_part, adapter_other)
    down_pair = jnp.where(first, adapter_other, adapter_part)
    gain_rows = lax.dynamic_slice_in_dim(gain_next[0], spot * pair, pair, 0).astype(jnp.float32)
    down_pair = (down_pair.astype(jnp.float32) * gain_rows[:, None]).astype(jnp.bfloat16)
    gain = jnp.where(first, norm_gain, gain_other).reshape(quads, blocks, LANES).astype(jnp.float32)

    by_side = frozen[0].reshape(quads, 2, 2, cols, cols)
    far_w = stage(by_side, static, chunks[2])
    other_w = swap(far_w)

    own_half = lax.dynamic_slice_in_dim(hidden_in, side * cols, cols, 1)
    other_half = swap(own_half)
    both = jnp.concatenate([jnp.where(first, own_half, other_half), jnp.where(first, other_half, own_half)], axis=1)
    source = both.reshape(units, rows, blocks, LANES).transpose(0, 2, 1, 3).reshape(units * blocks * rows, LANES)

    seg_hit = segment_ids[:, :, None] == lax.broadcasted_iota(jnp.int32, (1, 1, segment_job.shape[1]), 2)
    token_job = jnp.sum(jnp.where(seg_hit, segment_job[:, None, :], 0), axis=2)
    job_hit = token_job[:, :, None] == lax.broadcasted_iota(jnp.int32, (1, 1, job_adapter.shape[0]), 2)
    token_slot = jnp.sum(jnp.where(job_hit, job_adapter[None, None, :], 0), axis=2)
    slot = jnp.broadcast_to(token_slot.reshape(units * rows, 1), (units * rows, LANES))
    slot = lax.optimization_barrier(slot)

    smem = pl.BlockSpec(memory_space=pltpu.SMEM)
    vmem = pl.BlockSpec(memory_space=pltpu.VMEM)
    payload = jax.ShapeDtypeStruct((blocks * rows + SUB, LANES), jnp.bfloat16)
    partial = jax.ShapeDtypeStruct((2 * rows + 2 * SUB, cols), jnp.float32)
    out_shape = jax.ShapeDtypeStruct((units * rows, cols), jnp.bfloat16)
    early, late = (0, 1), (2, 3)

    def multiply(order, more, parity):
        return pl.pallas_call(
            functools.partial(partial_kernel, rows, order, more, parity),
            out_shape=partial,
            in_specs=[smem] + [vmem] * (len(order) + 3 + more),
            out_specs=vmem,
            compiler_params=pltpu.CompilerParams(vmem_limit_bytes=16 << 20),
            cost_estimate=pl.CostEstimate(
                flops=len(order) * 2 * rows * pair * pair, bytes_accessed=len(order) * 2 * pair * pair, transcendentals=0
            ),
            name="multiply",
        )

    def finish(parity):
        return pl.pallas_call(
            functools.partial(finish_kernel, rows, units, levels, 2 * half_width, parity),
            out_shape=(payload, out_shape),
            in_specs=[smem, smem] + [vmem] * 9,
            out_specs=(vmem, vmem),
            input_output_aliases={10: 1},
            compiler_params=pltpu.CompilerParams(vmem_limit_bytes=16 << 20),
            name="finish",
        )

    def end(step, parity, own_e, far_e, own_x, far_x, results):
        turn = jnp.full((1,), step, jnp.int32)
        return finish(parity)(static, turn, own_e, far_e, own_x, far_x, slot, up_pair, down_pair, source, results)

    def half_step(step, parity, far_edges, sent, results):
        def sends(p):
            return p % 2 == parity and (p % row != row - 1 or p in far_edges)

        blocks_in = {
            k: move(sent, route=lambda p, z, c, k=k: (p + 1, z + 2 * k + c, c) if sends(p) else None)
            for k in early + late
        }
        far_x = swap(blocks_in[0])
        weights = gain, *bring(by_side, other_w, static, sent, parity)
        own_e = multiply(early, False, parity)(static, *[blocks_in[k] for k in early], *weights)
        own_e = multiply(late, True, parity)(static, *[blocks_in[k] for k in late], *weights, own_e)
        far_e = swap(own_e)
        return end(step, parity, own_e, far_e, blocks_in[0], far_x, results)

    nothing_e = jnp.zeros(partial.shape, partial.dtype)
    nothing_x = jnp.zeros(payload.shape, payload.dtype)
    carry = end(-1, 0, nothing_e, nothing_e, nothing_x, nothing_x, jnp.zeros(out_shape.shape, out_shape.dtype))

    def two_steps(far_edges, i, carry):
        carry = half_step(2 * i, 1, far_edges, *carry)
        return half_step(2 * i + 1, 0, far_edges, *carry)

    turns = (levels + 2 * units - 2) // 2
    begin = 0
    while begin < turns:
        end_of = turns if begin >= levels // 2 else begin + (2 if begin else 4)
        far_edges = set()
        for p in range(row - 1, levels, row):
            first_turn = 0 if p == levels - 1 else (p + 1) // 2
            if first_turn < end_of and begin < first_turn + units:
                far_edges.add(p)
        carry = lax.fori_loop(begin, end_of, functools.partial(two_steps, far_edges), carry)
        begin = end_of
    return carry[1][None]


def solution(mesh):
    return jax.shard_map(
        relay,
        mesh=mesh,
        in_specs=(
            P(None, "tensor"),
            P(),
            P(),
            P(),
            P("section"),
            P("section", None, "tensor"),
            P("section", None),
            P("section", "tensor", None, None),
            P("section", "tensor", None, None),
        ),
        out_specs=P("section", None, "tensor"),
        check_vma=False,
    )
```

```python
import functools

import jax
import jax.numpy as jnp
from jax import lax
from jax.experimental import pallas as pl
from jax.experimental.pallas import tpu as pltpu
from jax.sharding import PartitionSpec as P

R = 32
LANES = 128
SUB = 8
epsilon = 1e-05
row = 4
AXES = ("section", "tensor")


def routed(value, levels, chips, route):
    def place(level, chip, core):
        section = 2 * (level % levels) + chip % 2
        return section * chips + (chip % chips) // 2 * 2 + core

    pairs = []
    for level in range(levels):
        for chip in range(chips):
            for core in range(2):
                target = route(level, chip, core)
                if target is not None:
                    pairs.append((place(level, chip, core), place(*target)))
    return lax.ppermute(value, AXES, pairs)


def bring(columns, far_w, static, sent, parity):
    quads, cores, _, cols, _ = columns.shape

    def kernel(static, columns, far_w, sent, out_a, out_b, done):
        copies = [pltpu.make_async_copy(far_w, out_b, done.at[quads * cores])]
        for q in range(quads):
            for core in range(cores):
                source = columns.at[q, core, static[6]]
                target = out_a.at[q, pl.ds(core * cols, cols), :]
                copies.append(pltpu.make_async_copy(source, target, done.at[q * cores + core]))

        @pl.when(static[5] & 1 != parity)
        def _():
            for copy in copies:
                copy.start()
            for copy in copies:
                copy.wait()

    held = pltpu.VMEM(far_w.shape, far_w.dtype)
    return pl.pallas_call(
        kernel,
        out_shape=(held, held),
        in_specs=[pl.BlockSpec(memory_space=pltpu.SMEM)] + [pl.BlockSpec(memory_space=pl.ANY)] * 3,
        out_specs=(pl.BlockSpec(memory_space=pltpu.VMEM),) * 2,
        scratch_shapes=[pltpu.SemaphoreType.DMA((quads * cores + 1,))],
        compiler_params=pltpu.CompilerParams(vmem_limit_bytes=1 << 20),
        cost_estimate=pl.CostEstimate(flops=1 << 32, bytes_accessed=4 * far_w.size, transcendentals=0),
        name="bring",
    )(static, columns, far_w, sent)


def stage(columns, static, after):
    quads, cores, _, cols, _ = columns.shape

    def kernel(static, columns, after, out, held, came, went):
        inward, outward = [], []
        for q in range(quads):
            for core in range(cores):
                i = q * cores + core
                rows_at = pl.ds(core * cols, cols)
                source = columns.at[q, core, 1 - static[6]]
                inward.append(pltpu.make_async_copy(source, held.at[q, rows_at, :], came.at[i]))
                outward.append(pltpu.make_async_copy(held.at[q, rows_at, :], out.at[q, rows_at, :], went.at[i]))
        for copy in inward:
            copy.start()
        for copy, onward in zip(inward, outward):
            copy.wait()
            onward.start()
        for onward in outward:
            onward.wait()

    return pl.pallas_call(
        kernel,
        out_shape=jax.ShapeDtypeStruct((quads, cores * cols, cols), columns.dtype),
        in_specs=[pl.BlockSpec(memory_space=pltpu.SMEM)] + [pl.BlockSpec(memory_space=pl.ANY)] * 2,
        out_specs=pl.BlockSpec(memory_space=pl.ANY),
        scratch_shapes=[
            pltpu.VMEM((quads, cores * cols, cols), columns.dtype),
            pltpu.SemaphoreType.DMA((quads * cores,)),
            pltpu.SemaphoreType.DMA((quads * cores,)),
        ],
        compiler_params=pltpu.CompilerParams(vmem_limit_bytes=8 << 20),
        cost_estimate=pl.CostEstimate(flops=1 << 32, bytes_accessed=columns.size, transcendentals=0),
        name="stage",
    )(static, columns, after)


def dot(left, right):
    return jnp.dot(left, right, preferred_element_type=jnp.float32)


def partial_kernel(rows, order, more, parity, static, *refs):
    @pl.when(static[5] & 1 != parity)
    def _():
        partial_body(rows, order, more, static, *refs)


def partial_body(rows, order, more, static, *refs):
    blocks_in, (gain, own_w, other_w), out = refs[: len(order)], refs[len(order) : len(order) + 3], refs[-1]
    core = static[4]
    cols = own_w.shape[2]
    blocks = 2 * cols // LANES
    own_sum = other_sum = squares = low = None
    for k, block in zip(order, blocks_in):
        place = static[k]
        parts = []
        for j in range(blocks):
            x = block[j * rows : (j + 1) * rows, :].astype(jnp.float32)
            squares = x * x if squares is None else squares + x * x
            parts.append((x * gain[place, j : j + 1, :]).astype(jnp.bfloat16))
        scaled = jnp.concatenate(parts, axis=1)
        low_k = block[blocks * rows :, :].astype(jnp.float32)
        own_k = dot(scaled, own_w[place])
        other_k = dot(scaled, other_w[place])
        own_sum = own_k if own_sum is None else own_sum + own_k
        other_sum = other_k if other_sum is None else other_sum + other_k
        low = low_k if low is None else low + low_k
    own_at = pl.ds(pl.multiple_of(core * rows, SUB), rows)
    other_at = pl.ds(pl.multiple_of((1 - core) * rows, SUB), rows)
    total = jnp.broadcast_to(jnp.sum(squares, axis=1, keepdims=True), (rows, LANES))
    if more:
        before = refs[len(order) + 3]
        own_sum = own_sum + before[own_at, :]
        other_sum = other_sum + before[other_at, :]
        low = low + before[2 * rows : 2 * rows + SUB, 0:LANES]
    out[own_at, :] = own_sum
    out[other_at, :] = other_sum
    out[2 * rows : 2 * rows + SUB, 0:LANES] = low
    for g in range(rows // SUB):
        at = slice(2 * rows + SUB, 2 * rows + 2 * SUB), slice(g * LANES, (g + 1) * LANES)
        part = total[g * SUB : (g + 1) * SUB]
        out[at] = part + before[at] if more else part


def finish_kernel(rows, units, levels, width, parity, static, *refs):
    @pl.when(static[5] & 1 != parity)
    def _():
        finish_body(rows, units, levels, width, static, *refs)


def finish_body(
    rows, units, levels, width, static, turn, own_e, far_e, own_x, far_x, slot, up, down, source, results_in, sent, results
):
    core, level = static[4], static[5]
    step = turn[0]
    cols = own_e.shape[1]
    blocks = 2 * cols // LANES
    groups = rows // SUB
    behind = step - level
    active = jnp.logical_and(behind >= 0, jnp.logical_and(behind < 2 * units, behind % 2 == 0))
    feeding = jnp.logical_and(level == levels - 1, jnp.logical_and(step % 2 != 0, step + 1 < 2 * units))
    unit = jnp.where(feeding, (step + 1) // 2, jnp.clip(behind // 2, 0, units - 1))
    at = pl.multiple_of(unit * rows, SUB)
    token_slot = slot[pl.ds(at, rows), :]
    lane_slot = lax.broadcasted_iota(jnp.int32, (SUB, LANES), 1) // R
    low = own_e[2 * rows : 2 * rows + SUB, 0:LANES] + far_e[2 * rows : 2 * rows + SUB, 0:LANES]
    turned = [low] + [pltpu.roll(low, s * R, 1) for s in range(1, 4)]
    scales, kept = [], []
    for g in range(groups):
        here = pl.ds(g * LANES, LANES)
        squares = own_e[2 * rows + SUB : 2 * rows + 2 * SUB, here] + far_e[2 * rows + SUB : 2 * rows + 2 * SUB, here]
        scale = lax.rsqrt(squares / width + epsilon)
        spread = turned[(0 - g) % 4]
        for a in range(1, 4):
            spread = jnp.where(lane_slot == a, turned[(a - g) % 4], spread)
        mine = lane_slot == token_slot[g * SUB : (g + 1) * SUB]
        kept.append(jnp.where(mine, spread * scale, 0.0))
        scales.append(scale)
    scale = jnp.concatenate(scales, axis=0)
    kept = jnp.concatenate(kept, axis=0).astype(jnp.bfloat16)
    fresh = []
    first = core == 0
    for j in range(blocks):
        row = j * rows
        x = jnp.where(first, own_x[row : row + rows, :], far_x[row : row + rows, :]).astype(jnp.float32)
        half, lane = (0, j * LANES) if j * LANES < cols else (rows, j * LANES - cols)
        product = own_e[half : half + rows, lane : lane + LANES] + far_e[half : half + rows, lane : lane + LANES]
        added = dot(kept, up[j * LANES : (j + 1) * LANES, :])
        y = (x + scale * product + added).astype(jnp.bfloat16)
        fed = source[pl.ds(pl.multiple_of(unit * (blocks * rows) + row, SUB), rows), :]
        fresh.append(jnp.where(feeding, fed, y))
    for j in range(blocks):
        sent[j * rows : (j + 1) * rows, :] = fresh[j]
    next_low = dot(jnp.concatenate(fresh, axis=1), down[...])
    packed = None
    for g in range(groups):
        mine = lane_slot == token_slot[g * SUB : (g + 1) * SUB]
        picked = jnp.where(mine, next_low[g * SUB : (g + 1) * SUB], 0.0)
        picked = picked + pltpu.roll(picked, 2 * R, 1)
        picked = picked + pltpu.roll(picked, R, 1)
        packed = picked if packed is None else jnp.where(lane_slot == g, picked, packed)
    sent[blocks * rows :, :] = packed.astype(jnp.bfloat16)

    @pl.when(active)
    def _():
        for i in range(blocks // 2):
            mine = jnp.where(first, fresh[i], fresh[blocks // 2 + i])
            results[pl.ds(at, rows), i * LANES : (i + 1) * LANES] = mine


def relay(
    hidden_in, segment_ids, segment_job, job_adapter, owner, frozen, norm_gain, inbox_down, inbox_up
):
    chips = lax.axis_size("tensor")
    levels = lax.axis_size("section") // 2
    cols = frozen.shape[2]
    half_width = norm_gain.shape[1]
    units, rows = segment_ids.shape
    quads = chips // 2
    pair = 2 * cols
    blocks = pair // LANES
    position = lax.axis_index("section")
    side, level = position & 1, position >> 1
    shard = lax.axis_index("tensor")
    spot, core = shard >> 1, shard & 1
    first = core == 0
    move = functools.partial(routed, levels=levels, chips=chips)

    def swap(value):
        return move(value, route=lambda p, z, c: (p, z, 1 - c))

    arriving = side ^ core
    places = [(spot - k - core * (1 - side)) & (quads - 1) for k in range(quads)]
    static = jnp.stack(places + [core, level, arriving]).astype(jnp.int32)

    down = inbox_down[0, 0]
    up = inbox_up[0, 0].reshape(LANES, half_width // LANES, LANES).transpose(1, 0, 2).reshape(half_width, LANES)
    from_core = swap(jnp.where(first, down, up))
    chip_has = jnp.where(owner[0] & 1 == core, jnp.where(first, up, down), from_core)
    owner_next = move(owner, route=lambda p, z, c: (p - 1, z, c))
    gain_next = move(norm_gain, route=lambda p, z, c: (p - 1, z, c))
    gain_other = move(norm_gain, route=lambda p, z, c: (p, z ^ 1, c))
    wanted = jnp.where(first, owner[0], owner_next[0]) >> 1
    adapter_part = None
    chunks = [lax.dynamic_slice_in_dim(chip_has, ((spot + k) & (quads - 1)) * pair, pair, 0) for k in range(quads)]
    for k in (2, 1, 3, 0):
        came = move(chunks[k], route=lambda p, z, c, k=k: (p - c, z + 2 * k, c))
        hit = (spot - k) & (quads - 1) == wanted
        adapter_part = came if adapter_part is None else jnp.where(hit, came, adapter_part)
    adapter_other = swap(adapter_part)
    up_pair = jnp.where(first, adapter_part, adapter_other)
    down_pair = jnp.where(first, adapter_other, adapter_part)
    gain_rows = lax.dynamic_slice_in_dim(gain_next[0], spot * pair, pair, 0).astype(jnp.float32)
    down_pair = (down_pair.astype(jnp.float32) * gain_rows[:, None]).astype(jnp.bfloat16)
    gain = jnp.where(first, norm_gain, gain_other).reshape(quads, blocks, LANES).astype(jnp.float32)

    by_side = frozen[0].reshape(quads, 2, 2, cols, cols)
    far_w = stage(by_side, static, chunks[2])
    other_w = swap(far_w)

    own_half = lax.dynamic_slice_in_dim(hidden_in, side * cols, cols, 1)
    other_half = swap(own_half)
    both = jnp.concatenate([jnp.where(first, own_half, other_half), jnp.where(first, other_half, own_half)], axis=1)
    source = both.reshape(units, rows, blocks, LANES).transpose(0, 2, 1, 3).reshape(units * blocks * rows, LANES)

    seg_hit = segment_ids[:, :, None] == lax.broadcasted_iota(jnp.int32, (1, 1, segment_job.shape[1]), 2)
    token_job = jnp.sum(jnp.where(seg_hit, segment_job[:, None, :], 0), axis=2)
    job_hit = token_job[:, :, None] == lax.broadcasted_iota(jnp.int32, (1, 1, job_adapter.shape[0]), 2)
    token_slot = jnp.sum(jnp.where(job_hit, job_adapter[None, None, :], 0), axis=2)
    slot = jnp.broadcast_to(token_slot.reshape(units * rows, 1), (units * rows, LANES))
    slot = lax.optimization_barrier(slot)

    smem = pl.BlockSpec(memory_space=pltpu.SMEM)
    vmem = pl.BlockSpec(memory_space=pltpu.VMEM)
    payload = jax.ShapeDtypeStruct((blocks * rows + SUB, LANES), jnp.bfloat16)
    partial = jax.ShapeDtypeStruct((2 * rows + 2 * SUB, cols), jnp.float32)
    out_shape = jax.ShapeDtypeStruct((units * rows, cols), jnp.bfloat16)
    arrivals = (0, 1), (2,), (3,)

    def multiply(order, more, parity):
        return pl.pallas_call(
            functools.partial(partial_kernel, rows, order, more, parity),
            out_shape=partial,
            in_specs=[smem] + [vmem] * (len(order) + 3 + more),
            out_specs=vmem,
            compiler_params=pltpu.CompilerParams(vmem_limit_bytes=16 << 20),
            cost_estimate=pl.CostEstimate(
                flops=len(order) * 2 * rows * pair * pair, bytes_accessed=len(order) * 2 * pair * pair, transcendentals=0
            ),
            name="multiply",
        )

    def finish(parity):
        return pl.pallas_call(
            functools.partial(finish_kernel, rows, units, levels, 2 * half_width, parity),
            out_shape=(payload, out_shape),
            in_specs=[smem, smem] + [vmem] * 9,
            out_specs=(vmem, vmem),
            input_output_aliases={10: 1},
            compiler_params=pltpu.CompilerParams(vmem_limit_bytes=16 << 20),
            name="finish",
        )

    def end(step, parity, own_e, far_e, own_x, far_x, results):
        turn = jnp.full((1,), step, jnp.int32)
        return finish(parity)(static, turn, own_e, far_e, own_x, far_x, slot, up_pair, down_pair, source, results)

    def half_step(step, parity, far_edges, sent, results):
        def sends(p):
            return p % 2 == parity and (p % row != row - 1 or p in far_edges)

        blocks_in = {
            k: move(sent, route=lambda p, z, c, k=k: (p + 1, z + 2 * k + c, c) if sends(p) else None)
            for k in range(quads)
        }
        far_x = swap(blocks_in[0])
        weights = gain, *bring(by_side, other_w, static, sent, parity)
        so_far = ()
        for ks in arrivals:
            blocks_now = [blocks_in[k] for k in ks]
            so_far = (multiply(ks, len(so_far), parity)(static, *blocks_now, *weights, *so_far),)
        (own_e,) = so_far
        far_e = swap(own_e)
        return end(step, parity, own_e, far_e, blocks_in[0], far_x, results)

    nothing_e = jnp.zeros(partial.shape, partial.dtype)
    nothing_x = jnp.zeros(payload.shape, payload.dtype)
    carry = end(-1, 0, nothing_e, nothing_e, nothing_x, nothing_x, jnp.zeros(out_shape.shape, out_shape.dtype))

    def two_steps(far_edges, i, carry):
        carry = half_step(2 * i, 1, far_edges, *carry)
        return half_step(2 * i + 1, 0, far_edges, *carry)

    turns = (levels + 2 * units - 2) // 2
    begin = 0
    while begin < turns:
        end_of = turns if begin >= levels // 2 else begin + (2 if begin else 4)
        far_edges = set()
        for p in range(row - 1, levels, row):
            first_turn = 0 if p == levels - 1 else (p + 1) // 2
            if first_turn < end_of and begin < first_turn + units:
                far_edges.add(p)
        carry = lax.fori_loop(begin, end_of, functools.partial(two_steps, far_edges), carry)
        begin = end_of
    return carry[1][None]


def solution(mesh):
    return jax.shard_map(
        relay,
        mesh=mesh,
        in_specs=(
            P(None, "tensor"),
            P(),
            P(),
            P(),
            P("section"),
            P("section", None, "tensor"),
            P("section", None),
            P("section", "tensor", None, None),
            P("section", "tensor", None, None),
        ),
        out_specs=P("section", None, "tensor"),
        check_vma=False,
    )
```
